32 devices in a mesh: px: 4 (over z), py: 2 (over y), sa: 4 (over x, core).
Axes of the slice: x: 2, y: 2, z: 4, core: 2. Of those that a mesh axis runs over, the one named last changes fastest.
Arguments:
- real_coeffs: float32 [4, 256, 256, 256], P('sa', 'px', 'py'), may hold values from -6 to 6
- imaginary_coeffs: float32 [4, 256, 256, 256], P('sa', 'px', 'py'), may hold values from -6 to 6
Outputs:
- modulus: float32 [4, 256, 256, 256], P(None, ('px', 'py'), 'sa')
The draws below stay inside these ranges and needn't reach their ends.
All inputs are finite; a program needn't handle non-finite values.
Results may differ from the reference program's by a relative error of at most 0.00007.
Values sent between devices are 32-bit elements; how exact they have to be, the bound alone decides.
A program may use at most 128 MiB of HBM per device.

```python
import math
import jax
import jax.numpy as jnp
from jax import lax

N = 256
SAMPLES = 4


def steps_of(stream_key, extent, pieces, smallest, top_value):
    loudness, own = 1.0, jax.random.fold_in(stream_key, 6)
    for dim, shards_of in pieces:
        steps = jnp.exp(jax.random.uniform(jax.random.fold_in(own, dim), (shards_of,), jnp.float32, smallest / len(pieces), top_value / len(pieces)))
        loudness = loudness * jnp.repeat(steps, extent[dim] // shards_of).reshape([-1 if axis == dim else 1 for axis in range(len(extent))])
    return loudness


def centred(rng, dims, scale, most, cuts=(), held_as=jnp.bfloat16):
    values = jax.random.normal(rng, dims, jnp.float32) * scale
    if len(cuts) > 0:
        values = steps_of(rng, dims, cuts, -0.22, 0.18) * values
    return jnp.clip(values, min=-most, max=most).astype(held_as)


def setup_inputs(seed: int = 0) -> dict:
    key_of = jax.random.split(jax.random.key(seed), 3)
    return {
        "real_coeffs": centred(key_of[0], (SAMPLES, N, N, N), 1.0, 6.0, ((0, 4), (1, 4), (2, 2)), jnp.float32),
        "imaginary_coeffs": centred(key_of[1], (SAMPLES, N, N, N), 1.0, 6.0, ((0, 4), (1, 4), (2, 2)), jnp.float32),
    }


corr_length = 1.0
log_spread = 0.5

def matern(squared, length):
    return 1.0 / (1.0 + (2.0 * math.pi * corr_length / length) ** 2 * squared)

def matern_scale(length):
    middle = length // 2
    square_counts = {}
    for position in range(length):
        square_value = ((position + middle) % length - middle) ** 2
        square_counts[square_value] = square_counts.get(square_value, 0) + 1
    plane_counts = {}
    for first_square, first_count in square_counts.items():
        for second_square, second_count in square_counts.items():
            plane_sum = first_square + second_square
            plane_counts[plane_sum] = plane_counts.get(plane_sum, 0) + first_count * second_count
    running = 0.0
    for first_square, first_count in square_counts.items():
        for plane_sum, plane_count in plane_counts.items():
            running = running + first_count * plane_count * matern(first_square + plane_sum, length) ** 2
    return 1.0 / math.sqrt(running)

def reference(real_coeffs, imaginary_coeffs):
    frequency = ((jnp.arange(N, dtype=jnp.int32) + N // 2) % N - N // 2).astype(jnp.float32)
    squared = frequency[:, None, None] ** 2 + frequency[None, :, None] ** 2 + frequency[None, None, :] ** 2
    weight = matern(squared, N) * matern_scale(N)

    def one_sample(coeff_pair):
        real_part = jnp.transpose(coeff_pair[0], (2, 0, 1))
        imag_part = jnp.transpose(coeff_pair[1], (2, 0, 1))
        spectrum = lax.complex(weight * real_part, weight * imag_part)
        log_field = jnp.real(jnp.fft.ifftn(spectrum)) * float(N ** 3)
        return jnp.exp(log_spread * log_field).astype(jnp.float32)
    return lax.map(one_sample, (real_coeffs, imaginary_coeffs))
```

```python
import math

import jax
import jax.numpy as jnp
import numpy as np
from jax import lax
from jax.experimental import pallas as pl
from jax.experimental.pallas import tpu as pltpu
from jax.sharding import PartitionSpec as P

corr_length = 1.0
log_spread = 0.5
CHUNKS = 4


def matern(squared, length):
    return 1.0 / (1.0 + (2.0 * math.pi * corr_length / length) ** 2 * squared)


def matern_scale(length):
    middle = length // 2
    squares = ((np.arange(length) + middle) % length - middle).astype(np.float64) ** 2
    plane = squares[:, None] + squares[None, :]
    running = 0.0
    for square in squares:
        running += float(np.sum(matern(square + plane, length) ** 2))
    return 1.0 / math.sqrt(running)


def signed(positions, length):
    return (positions + length // 2) % length - length // 2


def angles(length):
    places = np.arange(length)
    return (places[:, None] * places[None, :] % length) * (2.0 * math.pi / length)


def halves(table):
    high = jnp.asarray(table, jnp.float32).astype(jnp.bfloat16)
    low = (jnp.asarray(table, jnp.float32) - high.astype(jnp.float32)).astype(jnp.bfloat16)
    return high, low


def split(values):
    high = values.astype(jnp.bfloat16)
    return high, (values - high.astype(jnp.float32)).astype(jnp.bfloat16)


def product(first, second):
    (first_high, first_low), (second_high, second_low) = first, second
    dot = lambda one, two: jnp.dot(one, two, preferred_element_type=jnp.float32)
    return dot(first_high, second_high) + (dot(first_low, second_high) + dot(first_high, second_low))


def planes_kernel(z_high, z_low, y_high, y_low, lines, out):
    across, pieces, _, block, rows, columns = lines.shape
    length = across * rows
    for j in range(block):
        sides = []
        for part in range(2):
            sides += [
                lines[:, piece, part, j].reshape(length, columns) for piece in range(pieces)
            ]
        data = split(jnp.concatenate(sides, axis=1))
        mixed = product(data, (z_high[...], z_low[...]))
        stacked = split(jnp.concatenate([mixed[:, :length], mixed[:, length:]], axis=0))
        field = product((y_high[...], y_low[...]), stacked)
        values = jnp.exp(log_spread * field)
        out[:, j] = values.reshape(out.shape[0], out.shape[2], out.shape[3])


def planes(lines, tables, owners):
    across, pieces, _, count, rows, columns = lines.shape
    length = across * rows
    block = 1
    whole = lambda j: (0, 0)
    return pl.pallas_call(
        planes_kernel,
        grid=(count // block,),
        in_specs=[pl.BlockSpec(table.shape, whole) for table in tables]
        + [
            pl.BlockSpec(
                (across, pieces, 2, block, rows, columns), lambda j: (0, 0, 0, j, 0, 0)
            )
        ],
        out_specs=pl.BlockSpec(
            (owners, block, length // owners, length), lambda j: (0, j, 0, 0)
        ),
        out_shape=jax.ShapeDtypeStruct((owners, count, length // owners, length), jnp.float32),
        cost_estimate=pl.CostEstimate(
            flops=count * 36 * length**3, bytes_accessed=count * 12 * length**2,
            transcendentals=count * length**2,
        ),
    )(*tables, lines)


def local(real_coeffs, imaginary_coeffs):
    length = real_coeffs.shape[3]
    rows_y = real_coeffs.shape[1]
    rows_z = real_coeffs.shape[2]
    across_x = lax.axis_size("px")
    across_y = lax.axis_size("py")
    owners = lax.axis_size("sa")
    blocks = across_x * across_y
    depth = length // blocks
    chunks = math.gcd(CHUNKS, depth)
    thick = depth // chunks
    freq_x = signed(lax.iota(jnp.int32, length), length).astype(jnp.float32)
    freq_y = signed(lax.iota(jnp.int32, rows_y) + lax.axis_index("px") * rows_y, length).astype(
        jnp.float32
    )
    freq_z = signed(lax.iota(jnp.int32, rows_z) + lax.axis_index("py") * rows_z, length).astype(
        jnp.float32
    )
    squared = freq_x[None, None, :] ** 2 + freq_y[:, None, None] ** 2 + freq_z[None, :, None] ** 2
    weight = matern(squared, length) * matern_scale(length)
    real_in = real_coeffs[0] * weight
    imag_in = imaginary_coeffs[0] * weight

    theta = angles(length)
    cos, sin = np.cos(theta), np.sin(theta)
    tables = halves(np.block([[cos, sin], [-sin, cos]])) + halves(np.block([cos, -sin]))
    cos_x = cos.reshape(blocks, chunks, thick, length)
    sin_x = sin.reshape(blocks, chunks, thick, length)

    mine = lax.axis_index("sa")
    modulus = jnp.zeros((owners, depth, length // owners, length), jnp.float32)
    for chunk in range(chunks):
        on_real = np.stack([cos_x[:, chunk], sin_x[:, chunk]], axis=1).reshape(-1, length)
        on_imag = np.stack([-sin_x[:, chunk], cos_x[:, chunk]], axis=1).reshape(-1, length)
        mixed = jnp.einsum(
            "xk,abk->xab", jnp.asarray(on_real, jnp.float32), real_in, precision=lax.Precision.HIGH
        ) + jnp.einsum(
            "xk,abk->xab", jnp.asarray(on_imag, jnp.float32), imag_in, precision=lax.Precision.HIGH
        )
        mixed = mixed.reshape(blocks, 2 * thick * rows_y, rows_z)
        lines = lax.all_to_all(mixed, ("px", "py"), split_axis=0, concat_axis=0, tiled=True)
        lines = lines.reshape(across_x, across_y, 2, thick, rows_y, rows_z)
        if rows_z % 128:
            lines = lines.transpose(0, 2, 3, 4, 1, 5).reshape(
                across_x, 1, 2, thick, rows_y, length
            )
        field = planes(lines, tables, owners)
        for step in range(owners):
            piece = lax.dynamic_slice_in_dim(field, (mine + step) % owners, 1, 0)
            if step:
                ring = [(owner, (owner + step) % owners) for owner in range(owners)]
                piece = lax.ppermute(piece, "sa", ring)
            start = ((mine - step) % owners, chunk * thick, 0, 0)
            modulus = lax.dynamic_update_slice(modulus, piece, start)
    return modulus


def solution(mesh):
    placed = (P("sa", "px", "py", None), P("sa", "px", "py", None))
    return jax.shard_map(
        local,
        mesh=mesh,
        in_specs=placed,
        out_specs=P(None, ("px", "py"), "sa", None),
        check_vma=False,
    )
```

```python
import math

import jax
import jax.numpy as jnp
import numpy as np
from jax import lax
from jax.experimental import pallas as pl
from jax.experimental.pallas import tpu as pltpu
from jax.sharding import PartitionSpec as P

corr_length = 1.0
log_spread = 0.5


def matern(squared, length):
    return 1.0 / (1.0 + (2.0 * math.pi * corr_length / length) ** 2 * squared)


def matern_scale(length):
    middle = length // 2
    squares = ((np.arange(length) + middle) % length - middle).astype(np.float64) ** 2
    plane = squares[:, None] + squares[None, :]
    running = 0.0
    for square in squares:
        running += float(np.sum(matern(square + plane, length) ** 2))
    return 1.0 / math.sqrt(running)


def signed(positions, length):
    return (positions + length // 2) % length - length // 2


def angles(length):
    places = np.arange(length)
    return (places[:, None] * places[None, :] % length) * (2.0 * math.pi / length)


def halves(table):
    high = jnp.asarray(table, jnp.float32).astype(jnp.bfloat16)
    low = (jnp.asarray(table, jnp.float32) - high.astype(jnp.float32)).astype(jnp.bfloat16)
    return high, low


def split(values):
    high = values.astype(jnp.bfloat16)
    return high, (values - high.astype(jnp.float32)).astype(jnp.bfloat16)


def product(first, second):
    (first_high, first_low), (second_high, second_low) = first, second
    dot = lambda one, two: jnp.dot(one, two, preferred_element_type=jnp.float32)
    return dot(first_high, second_high) + (dot(first_low, second_high) + dot(first_high, second_low))


def lines_kernel(scale, starts, table, real_in, imag_in, out):
    _, tile, columns, length = real_in.shape
    middle = length // 2
    shape = (columns, length)
    wave_x = signed(lax.broadcasted_iota(jnp.int32, shape, 1), length).astype(jnp.float32)
    wave_z = signed(lax.broadcasted_iota(jnp.int32, shape, 0) + starts[1], length).astype(
        jnp.float32
    )
    base = wave_x**2 + wave_z**2
    rows = []
    for i in range(tile):
        place = starts[0] + pl.program_id(0) * tile + i
        wave_y = jnp.where(place >= middle, place - length, place)
        weight = matern(base + (wave_y * wave_y).astype(jnp.float32), length) * scale
        rows.append(jnp.concatenate([real_in[0, i] * weight, imag_in[0, i] * weight], axis=1))
    data_high, data_low = split(jnp.concatenate(rows, axis=0))
    dot = lambda one, two: lax.dot_general(
        one, two, (((1,), (1,)), ((), ())), preferred_element_type=jnp.float32
    )
    count = out.shape[0]
    both = dot(table[...], data_high)
    mixed = both[:count] + (both[count:] + dot(table[:count], data_low))
    for i in range(tile):
        out[:, i, :] = mixed[:, i * columns : (i + 1) * columns]


def x_lines(starts, table, real_coeffs, imaginary_coeffs, scale):
    _, rows_y, rows_z, length = real_coeffs.shape
    tile = math.gcd(rows_y, 8)
    count = table.shape[0] // 2
    side = pl.BlockSpec((1, tile, rows_z, length), lambda a: (0, a, 0, 0))
    whole = pl.BlockSpec(table.shape, lambda a: (0, 0))
    return pl.pallas_call(
        lambda *refs: lines_kernel(scale, *refs),
        grid=(rows_y // tile,),
        in_specs=[pl.BlockSpec(memory_space=pltpu.SMEM), whole, side, side],
        out_specs=pl.BlockSpec((count, tile, rows_z), lambda a: (0, a, 0)),
        out_shape=jax.ShapeDtypeStruct((count, rows_y, rows_z), jnp.float32),
        cost_estimate=pl.CostEstimate(
            flops=12 * count * rows_y * rows_z * length,
            bytes_accessed=4 * rows_y * rows_z * (2 * length + count),
            transcendentals=rows_y * rows_z * length,
        ),
    )(starts, table, real_coeffs, imaginary_coeffs)


def planes_kernel(high, low, lines, out):
    across, pieces, _, block, rows, columns = lines.shape
    length = across * rows
    for j in range(block):
        table = (high[...], low[...])
        sides = [
            jnp.concatenate(
                [lines[:, piece, part, j].reshape(length, columns) for piece in range(pieces)],
                axis=1,
            )
            for part in range(2)
        ]
        mixed = product(split(jnp.concatenate(sides, axis=0)), table)
        stacked = jnp.concatenate(
            [
                mixed[:length, :length] + mixed[length:, length:],
                mixed[length:, :length] - mixed[:length, length:],
            ],
            axis=0,
        )
        field = product(table, split(stacked))
        values = jnp.exp(log_spread * field)
        out[:, j] = values.reshape(out.shape[0], out.shape[2], out.shape[3])


def planes(lines, tables, owners):
    across, pieces, _, count, rows, columns = lines.shape
    length = across * rows
    block = 1
    whole = lambda j: (0, 0)
    return pl.pallas_call(
        planes_kernel,
        grid=(count // block,),
        in_specs=[pl.BlockSpec(table.shape, whole) for table in tables]
        + [
            pl.BlockSpec(
                (across, pieces, 2, block, rows, columns), lambda j: (0, 0, 0, j, 0, 0)
            )
        ],
        out_specs=pl.BlockSpec(
            (owners, block, length // owners, length), lambda j: (0, j, 0, 0)
        ),
        out_shape=jax.ShapeDtypeStruct((owners, count, length // owners, length), jnp.float32),
        cost_estimate=pl.CostEstimate(
            flops=count * 36 * length**3, bytes_accessed=count * 12 * length**2,
            transcendentals=count * length**2,
        ),
    )(*tables, lines)


def stage_sizes(depth):
    last = max(1, depth // 16)
    third = max(1, 3 * depth // 16)
    first = (depth - last - third) * 7 // 12
    return (first, depth - last - third - first, third, last)


def local(real_coeffs, imaginary_coeffs):
    length = real_coeffs.shape[3]
    rows_y = real_coeffs.shape[1]
    rows_z = real_coeffs.shape[2]
    across_x = lax.axis_size("px")
    across_y = lax.axis_size("py")
    owners = lax.axis_size("sa")
    blocks = across_x * across_y
    depth = length // blocks
    starts = jnp.stack([lax.axis_index("px") * rows_y, lax.axis_index("py") * rows_z])
    scale = matern_scale(length)
    theta = angles(length)
    cos, sin = np.cos(theta), np.sin(theta)
    table = halves(np.block([cos, -sin]))
    x_table = np.stack([np.block([cos, -sin]), np.block([sin, cos])])
    x_table = x_table.reshape(2, blocks, depth, 2 * length).transpose(1, 0, 2, 3)
    mine = lax.axis_index("sa")
    modulus = jnp.zeros((owners, depth, length // owners, length), jnp.float32)
    first = 0
    for thick in stage_sizes(depth):
        rows = x_table[:, :, first : first + thick].reshape(-1, 2 * length)
        mixed = x_lines(starts, jnp.concatenate(halves(rows)), real_coeffs, imaginary_coeffs, scale)
        mixed = mixed.reshape(blocks, 2 * thick * rows_y, rows_z)
        lines = lax.all_to_all(mixed, ("px", "py"), split_axis=0, concat_axis=0, tiled=True)
        lines = lines.reshape(across_x, across_y, 2, thick, rows_y, rows_z)
        if rows_z % 128:
            lines = lines.transpose(0, 2, 3, 4, 1, 5).reshape(
                across_x, 1, 2, thick, rows_y, length
            )
        field = planes(lines, table, owners)
        for step in range(owners):
            piece = lax.dynamic_slice_in_dim(field, (mine + step) % owners, 1, 0)
            if step:
                ring = [(owner, (owner + step) % owners) for owner in range(owners)]
                piece = lax.ppermute(piece, "sa", ring)
            start = ((mine - step) % owners, first, 0, 0)
            modulus = lax.dynamic_update_slice(modulus, piece, start)
        first += thick
    return modulus


def solution(mesh):
    placed = (P("sa", "px", "py", None), P("sa", "px", "py", None))
    return jax.shard_map(
        local,
        mesh=mesh,
        in_specs=placed,
        out_specs=P(None, ("px", "py"), "sa", None),
        check_vma=False,
    )
```
